128 devices in a mesh: prow: 16 (over y, x), pcol: 8 (over z, core).
Axes of the slice: x: 4, y: 4, z: 4, core: 2. Of those that a mesh axis runs over, the one named last changes fastest.
Arguments:
- u_window: float32 [6, 16, 512, 4, 8, 512], P(None, 'prow', None, None, 'pcol'), may hold values from -0.5 to 0.5
Outputs:
- lauum_columns: float32 [1024, 6, 16, 512], P('pcol', None, 'prow')
The draws below stay inside these ranges and needn't reach their ends.
All inputs are finite; a program needn't handle non-finite values.
Results may differ from the reference program's by a relative error of at most 0.000061.
Values sent between devices are 32-bit elements; how exact they have to be, the bound alone decides.
A program may use at most 192 MiB of HBM per device.

```python
import jax
import jax.numpy as jnp
from jax import lax

NB = 512
RB = 6
CB = 4
N_PROW = 16
N_PCOL = 8


def level_of(key, shape, split, least, top_value):
    gain, own = 1.0, jax.random.fold_in(key, 6)
    for axis_at, blocks in split:
        heights = jnp.exp(jax.random.uniform(jax.random.fold_in(own, axis_at), (blocks,), jnp.float32, least / len(split), top_value / len(split)))
        gain = gain * jnp.repeat(heights, shape[axis_at] // blocks).reshape([-1 if axis == axis_at else 1 for axis in range(len(shape))])
    return gain


def normal_values(key, dims, width, limit, cuts=(), held_as=jnp.bfloat16):
    values = width * jax.random.normal(key, dims, jnp.float32)
    if cuts:
        values = values * level_of(key, dims, cuts, -0.22, 0.18)
    return jnp.clip(values, -limit, limit).astype(held_as)


def setup_inputs(seed: int = 0) -> dict:
    splits = jax.random.split(jax.random.key(seed), 2)
    return {
        "u_window": normal_values(splits[0], (RB, N_PROW, NB, CB, N_PCOL, NB), ((CB * N_PCOL * NB) ** -0.25), 0.5, ((1, 16), (4, 8)), jnp.float32),
    }


def contract(left, right):
    return lax.dot_general(left, right, (((1,), (1,)), ((), ())), precision=lax.Precision.HIGHEST, preferred_element_type=jnp.float32)


def reference(u_window):
    height = RB * N_PROW
    width_cols = CB * N_PCOL * NB
    matrix = u_window.reshape(height * NB, width_cols)
    anchor = (height - 2) * NB
    panel_rows = matrix[anchor:]
    row_ids = jnp.arange(2 * NB, dtype=jnp.int32)
    col_ids = jnp.arange(width_cols, dtype=jnp.int32)
    masked = jnp.where(row_ids[:, None] <= col_ids[None, :], panel_rows, jnp.zeros_like(panel_rows))
    product = jnp.concatenate([contract(masked, matrix[:anchor]), contract(masked, masked)], 1)
    return product.reshape(2 * NB, RB, N_PROW, NB)
```

```python
import functools

import jax
import jax.numpy as jnp
from jax import lax
from jax.experimental import pallas as pl
from jax.experimental.pallas import tpu as pltpu
from jax.sharding import PartitionSpec as P

MESH = pl.DeviceIdType.MESH
ROWS = 16
SPLIT = 2
SLOTS = 3
LAG = 4


def gray(index):
    return index ^ (index >> 1)


def address(row):
    return gray(row // 4) * 4 + gray(row % 4)


def parents(tree):
    order = [(tree + k + 1) % 4 for k in range(4)]
    order = ([(tree - k - 1) % 4 for k in range(4)])[::-1]
    found = {}
    for node in range(1, 16):
        rest = node ^ (1 << tree)
        found[node] = 0 if rest == 0 else node ^ (1 << [d for d in order if rest >> d & 1][0])
    return found


def plans(n_rows, sources):
    trees = [parents(tree) for tree in range(4)]
    taken = set()
    for tree in trees:
        for node, parent in tree.items():
            assert (parent, node) not in taken
            taken.add((parent, node))
    result = []
    for row in range(n_rows):
        pieces = []
        for index, source in enumerate(sources):
            me = address(row) ^ address(source)
            for number, tree in enumerate(trees):
                depth, node = 0, me
                while node:
                    depth, node = depth + 1, tree[node]
                mask = sum(1 << d for d in range(4) if tree.get(me ^ (1 << d)) == me)
                pieces.append((depth, index * 4 + number, mask))
        result.append(sorted(pieces))
    return result


def kernel(
    x_ref,
    out_ref,
    high,
    low,
    panel,
    left,
    part,
    fold,
    mid,
    last,
    stage,
    in_sem,
    go_sem,
    fold_send,
    fold_recv,
    mid_send,
    mid_recv,
    last_send,
    last_recv,
    out_sem,
    stage_sem,
    *,
    n_row,
    n_col,
):
    p = lax.axis_index("prow")
    q = lax.axis_index("pcol")
    z, c = q // 2, q % 2
    n_block, depth, block = high.shape
    lanes = depth // 128
    per_block = block // 128
    n_stage = n_block * per_block
    n_set = panel.shape[0]
    n_step = n_set * SPLIT
    width = part.shape[2]
    half = part.shape[1] // 2
    first_source = n_row - 2
    anchor = n_row * n_block - 2

    x, y = p % 4, p // 4
    near = [
        y * 4 + x + 1 - 2 * (x % 2),
        y * 4 + 3 - x,
        (y + 1 - 2 * (y % 2)) * 4 + x,
        (3 - y) * 4 + x,
    ]
    peer = q + 1 - 2 * c
    up = ((z + 1) % 4) * 2 + c
    down = ((z + 3) % 4) * 2 + c

    def pick(values):
        found = jnp.int32(values[0])
        for k in range(1, n_row):
            found = jnp.where(p == k, jnp.int32(values[k]), found)
        return found

    plan = plans(n_row, (first_source, first_source + 1))
    routes = [
        pick([sum((e[1] + 8 * e[2]) << 7 * k for k, e in enumerate(row[g : g + 4])) for row in plan])
        for g in (0, 4)
    ]
    depths = [
        pick([sum(e[0] << 3 * k for k, e in enumerate(row[g : g + 4])) for row in plan])
        for g in (0, 4)
    ]

    def place(piece):
        return pl.multiple_of(((piece % 2) * 4 + piece // 2) * (ROWS * lanes), ROWS * lanes)

    def piece_ref(s, piece):
        return panel.at[s, pl.ds(place(piece), ROWS * lanes), :]

    def stage_copy(n):
        slot = n % SLOTS
        return pltpu.make_async_copy(
            x_ref.at[pl.ds(pl.multiple_of(n * (128 * lanes), 128 * lanes), 128 * lanes), :],
            stage.at[slot],
            stage_sem.at[slot],
        )

    for n in range(SLOTS):
        stage_copy(n).start()

    @pl.when(p >= first_source)
    def _():
        def own(s, _):
            for t in range(4):
                piece = (p - first_source) * 4 + t
                row = (n_block - 1) * block + t * 128 + s * ROWS
                pltpu.make_async_copy(
                    x_ref.at[pl.ds(pl.multiple_of(row * lanes, ROWS * lanes), ROWS * lanes), :],
                    piece_ref(s, piece),
                    in_sem.at[s, piece],
                ).start()
            return 0

        lax.fori_loop(0, n_set, own, 0)

    barrier = pltpu.get_barrier_semaphore()
    partners = [(row, q) for row in near] + [(p, peer), (p, up), (p, down)]
    for partner in partners:
        pl.semaphore_signal(barrier, inc=1, device_id=partner, device_id_type=MESH)
    pl.semaphore_wait(barrier, len(partners))

    def prepare(n, _):
        slot = n % SLOTS
        stage_copy(n).wait()
        row_id = (
            ((n // per_block) * n_row + p - anchor) * block
            + (n % per_block) * 128
            + lax.broadcasted_iota(jnp.int32, (128, 128), 1)
        )
        for j in range(lanes):
            value = stage[slot, pl.ds(j, 128, stride=lanes), :].T
            first_col = (j // per_block * n_col + q) * block + j % per_block * 128
            if j < per_block:
                col_id = first_col + lax.broadcasted_iota(jnp.int32, (128, 128), 0)
                value = jnp.where(row_id <= col_id, value, 0.0)
            top = value.astype(jnp.bfloat16)
            at = (n // per_block, pl.ds(j * 128, 128), pl.ds(pl.multiple_of(n % per_block * 128, 128), 128))
            high[at] = top
            low[at] = (value - top.astype(jnp.float32)).astype(jnp.bfloat16)

        @pl.when(n + SLOTS < n_stage)
        def _():
            stage_copy(n + SLOTS).start()

        return 0

    def relay(s, done, pace):
        for group in range(2):

            def one(j, carry):
                route, far, done = carry
                piece, mask = route % 8, route // 8 % 16
                if pace:
                    goal = jnp.minimum(far % 8 * pace, n_stage)
                    goal = jnp.maximum(goal, done)
                    lax.fori_loop(done, goal, prepare, 0)
                    done = goal
                ref = piece_ref(s, piece)
                pltpu.make_async_copy(ref, ref, in_sem.at[s, piece]).wait()
                for d in range(4):

                    @pl.when(mask // (1 << d) % 2 == 1)
                    def _():
                        slot = go_sem.at[group * 4 + j, d]

                        @pl.when(s > 0)
                        def _():
                            pltpu.make_async_copy(ref, ref, slot).wait()

                        pltpu.make_async_remote_copy(
                            src_ref=ref,
                            dst_ref=ref,
                            send_sem=slot,
                            recv_sem=in_sem.at[s, piece],
                            device_id=(near[d], q),
                            device_id_type=MESH,
                        ).start()

                return route // 128, far // 8, done

            done = lax.fori_loop(0, 4, one, (routes[group], depths[group], done))[2]
        return done

    def split_panel(s):
        row = lax.broadcasted_iota(jnp.int32, (8 * ROWS, 128), 0)
        place_of, within = row // ROWS, row % ROWS
        row_id = (place_of % 4 * 2 + place_of // 4) * 128 + s * ROWS + within
        for j in range(lanes):
            value = panel[s, pl.ds(j, 8 * ROWS, stride=lanes), :]
            if j < per_block:
                col_id = q * block + j * 128 + lax.broadcasted_iota(jnp.int32, (8 * ROWS, 128), 1)
                value = jnp.where(row_id <= col_id, value, 0.0)
            top = value.astype(jnp.bfloat16)
            left[: 8 * ROWS, j * 128 : j * 128 + 128] = top
            left[8 * ROWS :, j * 128 : j * 128 + 128] = (value - top.astype(jnp.float32)).astype(
                jnp.bfloat16
            )

    def fold_copy(t):
        return pltpu.make_async_remote_copy(
            src_ref=part.at[t, pl.ds(pl.multiple_of((1 - c) * half, half), half), :],
            dst_ref=fold.at[t],
            send_sem=fold_send.at[t],
            recv_sem=fold_recv.at[t],
            device_id=(p, peer),
            device_id_type=MESH,
        )

    def rows_of(zone, offset):
        return pl.multiple_of(c * half + zone * ROWS + offset, 8)

    def mid_copy(t, way):
        start = rows_of((z + 2) % 4, way * (ROWS // 2))
        return pltpu.make_async_remote_copy(
            src_ref=part.at[t, pl.ds(start, ROWS // 2), :],
            dst_ref=mid.at[t, way],
            send_sem=mid_send.at[t, way],
            recv_sem=mid_recv.at[t, way],
            device_id=(p, (up, down)[way]),
            device_id_type=MESH,
        )

    def last_copy(t, way):
        start = rows_of((z + (1, 3)[way]) % 4, 0)
        return pltpu.make_async_remote_copy(
            src_ref=part.at[t, pl.ds(start, ROWS), :],
            dst_ref=last.at[t, way],
            send_sem=last_send.at[t, way],
            recv_sem=last_recv.at[t, way],
            device_id=(p, (up, down)[way]),
            device_id_type=MESH,
        )

    def out_copy(t):
        return pltpu.make_async_copy(
            part.at[t, pl.ds(rows_of(z, 0), ROWS), :],
            out_ref.at[
                pl.ds(pl.multiple_of(t // SPLIT * ROWS, ROWS), ROWS),
                pl.ds(pl.multiple_of(t % SPLIT * width, width), width),
            ],
            out_sem.at[t],
        )

    def compute(t):
        s, h = t // SPLIT, t % SPLIT
        for i in range(n_block // SPLIT):
            at = h * (n_block // SPLIT) + i
            both = jnp.dot(left[...], high[at], preferred_element_type=jnp.float32)
            rest = jnp.dot(left[: 8 * ROWS], low[at], preferred_element_type=jnp.float32)
            part[t, :, i * block : (i + 1) * block] = both[: 8 * ROWS] + both[8 * ROWS :] + rest

    def add_fold(t):
        fold_copy(t).wait_recv()
        for r in range(0, half, 8):
            at = (t, pl.ds(pl.multiple_of(c * half + r, 8), 8), slice(None))
            part[at] = part[at] + fold[t, r : r + 8, :]
        for way in range(2):
            mid_copy(t, way).start()

    def add_mid(t):
        for way in range(2):
            mid_copy(t, way).wait_recv()
            at = (t, pl.ds(rows_of((z + (1, 3)[way]) % 4, way * (ROWS // 2)), ROWS // 2), slice(None))
            part[at] = part[at] + mid[t, way]
        for way in range(2):
            last_copy(t, way).start()

    def add_last(t):
        for way in range(2):
            last_copy(t, way).wait_recv()
        for r in range(0, ROWS, 8):
            at = (t, pl.ds(rows_of(z, r), 8), slice(None))
            part[at] = part[at] + last[t, 0, r : r + 8, :] + last[t, 1, r : r + 8, :]
        out_copy(t).start()

    done = relay(0, jnp.int32(0), 8)
    lax.fori_loop(done, n_stage, prepare, 0)

    def step(t, _):
        @pl.when(t < n_step)
        def _():
            @pl.when(t % SPLIT == 0)
            def _():
                s = t // SPLIT

                @pl.when(s > 0)
                def _():
                    relay(s, jnp.int32(0), 0)

                split_panel(s)

            compute(t)
            fold_copy(t).start()

        for lag, work in ((1, add_fold), (2, add_mid), (LAG, add_last)):

            @pl.when((t >= lag) & (t < n_step + lag))
            def _():
                work(t - lag)

        return 0

    lax.fori_loop(0, n_step + LAG, step, 0)

    def finish(t, _):
        fold_copy(t).wait_send()
        for way in range(2):
            mid_copy(t, way).wait_send()
            last_copy(t, way).wait_send()
        out_copy(t).wait()
        return 0

    lax.fori_loop(0, n_step, finish, 0)
    for group in range(2):

        def spent(j, route):
            ref = piece_ref(0, route % 8)
            for d in range(4):

                @pl.when(route // 8 % 16 // (1 << d) % 2 == 1)
                def _():
                    pltpu.make_async_copy(ref, ref, go_sem.at[group * 4 + j, d]).wait()

            return route // 128

        lax.fori_loop(0, 4, spent, routes[group])


def on_device(u_window):
    n_block, _, block, col_blocks, _, _ = u_window.shape
    n_row, n_col = lax.axis_size("prow"), lax.axis_size("pcol")
    depth = col_blocks * block
    lanes = depth // 128
    height = n_block * block
    width = height // SPLIT
    n_set = 128 // ROWS
    n_step = n_set * SPLIT
    dma = pltpu.SemaphoreType.DMA
    summed = pl.pallas_call(
        functools.partial(kernel, n_row=n_row, n_col=n_col),
        out_shape=jax.ShapeDtypeStruct((2 * block // n_col, height), jnp.float32),
        in_specs=[pl.BlockSpec(memory_space=pl.ANY)],
        out_specs=pl.BlockSpec(memory_space=pl.ANY),
        scratch_shapes=[
            pltpu.VMEM((n_block, depth, block), jnp.bfloat16),
            pltpu.VMEM((n_block, depth, block), jnp.bfloat16),
            pltpu.VMEM((n_set, 8 * ROWS * lanes, 128), jnp.float32),
            pltpu.VMEM((16 * ROWS, depth), jnp.bfloat16),
            pltpu.VMEM((n_step, 8 * ROWS, width), jnp.float32),
            pltpu.VMEM((n_step, 4 * ROWS, width), jnp.float32),
            pltpu.VMEM((n_step, 2, ROWS // 2, width), jnp.float32),
            pltpu.VMEM((n_step, 2, ROWS, width), jnp.float32),
            pltpu.VMEM((SLOTS, 128 * lanes, 128), jnp.float32),
            dma((n_set, 8)),
            dma((8, 4)),
            dma((n_step,)),
            dma((n_step,)),
            dma((n_step, 2)),
            dma((n_step, 2)),
            dma((n_step, 2)),
            dma((n_step, 2)),
            dma((n_step,)),
            dma((SLOTS,)),
        ],
        compiler_params=pltpu.CompilerParams(
            collective_id=0, has_side_effects=True, vmem_limit_bytes=67043328
        ),
    )(u_window.reshape(height * lanes, 128))
    return summed.reshape(summed.shape[0], n_block, 1, block)


def solution(mesh):
    placed = (P(None, "prow", None, None, "pcol", None),)
    return jax.shard_map(
        on_device,
        mesh=mesh,
        in_specs=placed,
        out_specs=P("pcol", None, "prow", None),
        check_vma=False,
    )
```

```python
import functools

import jax
import jax.numpy as jnp
from jax import lax
from jax.experimental import pallas as pl
from jax.experimental.pallas import tpu as pltpu
from jax.sharding import PartitionSpec as P

MESH = pl.DeviceIdType.MESH
ROWS = 16
PIECE = 8
TURNS = 3
DELAY = (0, 4, 8, 12, 16, 20)
SPLIT = 2
SLOTS = 3
LAGS = (1, 2, 4)


def gray(index):
    return index ^ (index >> 1)


def address(row):
    return gray(row // 4) * 4 + gray(row % 4)


def parents(tree):
    order = [(tree + k + 1) % 4 for k in range(4)]
    order = ([(tree - k - 1) % 4 for k in range(4)])[::-1]
    found = {}
    for node in range(1, 16):
        rest = node ^ (1 << tree)
        found[node] = 0 if rest == 0 else node ^ (1 << [d for d in order if rest >> d & 1][0])
    return found


def plans(n_rows, sources):
    trees = [parents(tree) for tree in range(4)]
    taken = set()
    for tree in trees:
        for node, parent in tree.items():
            assert (parent, node) not in taken
            taken.add((parent, node))
    result = []
    for row in range(n_rows):
        pieces = []
        for index, source in enumerate(sources):
            me = address(row) ^ address(source)
            for number, tree in enumerate(trees):
                depth, node = 0, me
                while node:
                    depth, node = depth + 1, tree[node]
                mask = sum(1 << d for d in range(4) if tree.get(me ^ (1 << d)) == me)
                pieces.append((depth, index * 4 + number, mask))
        result.append(sorted(pieces))
    return result


def kernel(
    x_ref,
    out_ref,
    high,
    low,
    panel,
    left,
    part,
    fold,
    mid,
    last,
    stage,
    flat,
    in_sem,
    go_sem,
    fold_send,
    fold_recv,
    mid_send,
    mid_recv,
    last_send,
    last_recv,
    out_sem,
    stage_sem,
    *,
    n_row,
    n_col,
):
    p = lax.axis_index("prow")
    q = lax.axis_index("pcol")
    z, c = q // 2, q % 2
    n_block, depth, block = high.shape
    lanes = depth // 128
    per_block = block // 128
    n_stage = n_block * per_block
    n_wave = panel.shape[0]
    n_set = n_wave // (ROWS // PIECE)
    n_step = n_set * SPLIT
    width = part.shape[2]
    half = part.shape[1] // 2
    first_source = n_row - 2
    anchor = n_row * n_block - 2

    x, y = p % 4, p // 4
    near = [
        y * 4 + x + 1 - 2 * (x % 2),
        y * 4 + 3 - x,
        (y + 1 - 2 * (y % 2)) * 4 + x,
        (3 - y) * 4 + x,
    ]
    peer = q + 1 - 2 * c
    up = ((z + 1) % 4) * 2 + c
    down = ((z + 3) % 4) * 2 + c

    def pick(values):
        found = jnp.int32(values[0])
        for k in range(1, n_row):
            found = jnp.where(p == k, jnp.int32(values[k]), found)
        return found

    plan = plans(n_row, (first_source, first_source + 1))
    moves = []
    for k in range(8):
        piece = pick([row[k][1] for row in plan])
        mask = pick([row[k][2] for row in plan])
        late = pick([DELAY[row[k][0]] for row in plan])
        start = pl.multiple_of((piece % 2 * 4 + piece // 2) * (PIECE * lanes), PIECE * lanes)
        turn = [late % TURNS == i for i in range(TURNS)]
        sends = [mask // (1 << d) % 2 == 1 for d in range(4)]
        moves.append((piece, start, late // TURNS, turn, sends))

    ahead = -(-(DELAY[-1] + TURNS * (ROWS // PIECE - 1)) // TURNS)
    size = PIECE * lanes

    def piece_ref(u, start):
        return panel.at[u, pl.ds(start, size), :]

    def stage_copy(n):
        slot = n % SLOTS
        return pltpu.make_async_copy(
            x_ref.at[pl.ds(pl.multiple_of(n * (128 * lanes), 128 * lanes), 128 * lanes), :],
            stage.at[slot],
            stage_sem.at[slot],
        )

    for n in range(SLOTS):
        stage_copy(n).start()

    @pl.when(p >= first_source)
    def _():
        def own(u, _):
            for t in range(4):
                piece = (p - first_source) * 4 + t
                start = pl.multiple_of((t % 2 * 4 + (p - first_source) * 2 + t // 2) * size, size)
                row = (n_block - 1) * block + t * 128 + u * PIECE
                pltpu.make_async_copy(
                    x_ref.at[pl.ds(pl.multiple_of(row * lanes, size), size), :],
                    piece_ref(u, start),
                    in_sem.at[u, piece],
                ).start()
            return 0

        lax.fori_loop(0, n_wave, own, 0)

    barrier = pltpu.get_barrier_semaphore()
    partners = [(row, q) for row in near] + [(p, peer), (p, up), (p, down)]
    for partner in partners:
        pl.semaphore_signal(barrier, inc=1, device_id=partner, device_id_type=MESH)
    pl.semaphore_wait(barrier, len(partners))

    def prepare(n, _):
        slot = n % SLOTS
        stage_copy(n).wait()
        row_id = (
            ((n // per_block) * n_row + p - anchor) * block
            + (n % per_block) * 128
            + lax.broadcasted_iota(jnp.int32, (128, 128), 1)
        )
        for j in range(lanes):
            value = stage[slot, pl.ds(j, 128, stride=lanes), :].T
            first_col = (j // per_block * n_col + q) * block + j % per_block * 128
            if j < per_block:
                col_id = first_col + lax.broadcasted_iota(jnp.int32, (128, 128), 0)
                value = jnp.where(row_id <= col_id, value, 0.0)
            top = value.astype(jnp.bfloat16)
            at = (n // per_block, pl.ds(j * 128, 128), pl.ds(pl.multiple_of(n % per_block * 128, 128), 128))
            high[at] = top
            low[at] = (value - top.astype(jnp.float32)).astype(jnp.bfloat16)

        @pl.when(n + SLOTS < n_stage)
        def _():
            stage_copy(n + SLOTS).start()

        return 0

    def relay(slot, i):
        for piece, start, late, turn, sends in moves:
            u = slot - late

            @pl.when(turn[i] & (u >= 0) & (u < n_wave))
            def _():
                ref = piece_ref(u, start)
                pltpu.make_async_copy(ref, ref, in_sem.at[u, piece]).wait()
                for d in range(4):

                    @pl.when(sends[d])
                    def _():
                        pltpu.make_async_remote_copy(
                            src_ref=ref,
                            dst_ref=ref,
                            send_sem=go_sem.at[piece // 4, d],
                            recv_sem=in_sem.at[u, piece],
                            device_id=(near[d], q),
                            device_id_type=MESH,
                        ).start()

    def split_panel(s):
        row = lax.broadcasted_iota(jnp.int32, (8 * ROWS, 128), 0)
        place_of, within = row // ROWS, row % ROWS
        row_id = (place_of % 4 * 2 + place_of // 4) * 128 + s * ROWS + within
        for j in range(lanes):
            waves = [
                panel[s * (ROWS // PIECE) + w, pl.ds(j, 8 * PIECE, stride=lanes), :]
                for w in range(ROWS // PIECE)
            ]
            value = jnp.concatenate(
                [wave[g * PIECE : g * PIECE + PIECE] for g in range(8) for wave in waves], 0
            )
            if j < per_block:
                col_id = q * block + j * 128 + lax.broadcasted_iota(jnp.int32, (8 * ROWS, 128), 1)
                value = jnp.where(row_id <= col_id, value, 0.0)
            top = value.astype(jnp.bfloat16)
            left[: 8 * ROWS, j * 128 : j * 128 + 128] = top
            left[8 * ROWS :, j * 128 : j * 128 + 128] = (value - top.astype(jnp.float32)).astype(
                jnp.bfloat16
            )

    def fold_copy(t):
        return pltpu.make_async_remote_copy(
            src_ref=part.at[t, pl.ds(pl.multiple_of((1 - c) * half, half), half), :],
            dst_ref=fold.at[t],
            send_sem=fold_send.at[0],
            recv_sem=fold_recv.at[t],
            device_id=(p, peer),
            device_id_type=MESH,
        )

    def rows_of(zone, offset):
        return pl.multiple_of(c * half + zone * ROWS + offset, 8)

    def mid_copy(t, way):
        start = rows_of((z + 2) % 4, way * (ROWS // 2))
        return pltpu.make_async_remote_copy(
            src_ref=part.at[t, pl.ds(start, ROWS // 2), :],
            dst_ref=mid.at[t, way],
            send_sem=mid_send.at[way],
            recv_sem=mid_recv.at[t, way],
            device_id=(p, (up, down)[way]),
            device_id_type=MESH,
        )

    def last_copy(t, way):
        start = rows_of((z + (1, 3)[way]) % 4, 0)
        return pltpu.make_async_remote_copy(
            src_ref=part.at[t, pl.ds(start, ROWS), :],
            dst_ref=last.at[t, way],
            send_sem=last_send.at[way],
            recv_sem=last_recv.at[t, way],
            device_id=(p, (up, down)[way]),
            device_id_type=MESH,
        )

    def out_copy(s):
        rows = ROWS * n_block * per_block
        ref = pl.ds(pl.multiple_of(s * rows, rows), rows)
        return pltpu.make_async_copy(flat.at[ref, :], out_ref.at[ref, :], out_sem.at[0])

    def compute(t, h, i):
        at = h * (n_block // SPLIT) + i
        both = jnp.dot(left[...], high[at], preferred_element_type=jnp.float32)
        rest = jnp.dot(left[: 8 * ROWS], low[at], preferred_element_type=jnp.float32)
        part[t, :, i * block : (i + 1) * block] = both[: 8 * ROWS] + both[8 * ROWS :] + rest

    def add_fold(t):
        fold_copy(t).wait_recv()
        for r in range(0, half, 8):
            at = (t, pl.ds(pl.multiple_of(c * half + r, 8), 8), slice(None))
            part[at] = part[at] + fold[t, r : r + 8, :]
        for way in range(2):
            mid_copy(t, way).start()

    def add_mid(t):
        for way in range(2):
            mid_copy(t, way).wait_recv()
            at = (t, pl.ds(rows_of((z + (1, 3)[way]) % 4, way * (ROWS // 2)), ROWS // 2), slice(None))
            part[at] = part[at] + mid[t, way]
        for way in range(2):
            last_copy(t, way).start()

    def add_last(t):
        for way in range(2):
            last_copy(t, way).wait_recv()
        s, h = t // SPLIT, t % SPLIT
        for j in range(width // 128):
            cols = slice(j * 128, j * 128 + 128)
            value = part[t, pl.ds(rows_of(z, 0), ROWS), cols] + last[t, 0, :, cols] + last[t, 1, :, cols]
            first = s * (ROWS * n_block * per_block) + h * (width // 128) + j
            flat[pl.ds(first, ROWS, stride=n_block * per_block), :] = value

        @pl.when(h == SPLIT - 1)
        def _():
            out_copy(s).start()

    share = -(-n_stage // (ahead * TURNS))

    def fill(slot, _):
        for i in range(TURNS):
            relay(slot, i)
            first = (slot * TURNS + i) * share
            lax.fori_loop(first, jnp.minimum(first + share, n_stage), prepare, 0)
        return 0

    lax.fori_loop(0, ahead, fill, 0)

    def sums(t, work, lag):
        @pl.when((t >= lag) & (t < n_step + lag))
        def _():
            work(t - lag)

    def one_set(s, _):
        for h in range(SPLIT):
            t = s * SPLIT + h
            for i in range(TURNS):
                relay(t + ahead, i)
                if h == 0 and i == 0:
                    split_panel(s)
                compute(t, h, i)
                if i == 1:
                    sums(t, add_fold, LAGS[0])
            fold_copy(t).start()
            sums(t, add_mid, LAGS[1])
            sums(t, add_last, LAGS[2])
        return 0

    lax.fori_loop(0, n_set, one_set, 0)

    def drain(t, _):
        for work, lag in zip((add_fold, add_mid, add_last), LAGS):
            sums(t, work, lag)
        return 0

    lax.fori_loop(n_step, n_step + LAGS[2], drain, 0)
    pltpu.make_async_copy(fold, fold, fold_send.at[0]).wait()
    for way in range(2):
        ref = mid.at[:, way]
        pltpu.make_async_copy(ref, ref, mid_send.at[way]).wait()
        ref = last.at[:, way]
        pltpu.make_async_copy(ref, ref, last_send.at[way]).wait()
    ref = panel.at[:, pl.ds(0, size), :]
    for piece, _, _, _, sends in moves:
        for d in range(4):

            @pl.when(sends[d])
            def _():
                pltpu.make_async_copy(ref, ref, go_sem.at[piece // 4, d]).wait()

    pltpu.make_async_copy(flat, flat, out_sem.at[0]).wait()


def on_device(u_window):
    n_block, _, block, col_blocks, _, _ = u_window.shape
    n_row, n_col = lax.axis_size("prow"), lax.axis_size("pcol")
    depth = col_blocks * block
    lanes = depth // 128
    height = n_block * block
    width = height // SPLIT
    n_set = 128 // ROWS
    n_step = n_set * SPLIT
    n_wave = n_set * (ROWS // PIECE)
    dma = pltpu.SemaphoreType.DMA
    summed = pl.pallas_call(
        functools.partial(kernel, n_row=n_row, n_col=n_col),
        out_shape=jax.ShapeDtypeStruct((2 * block // n_col * (height // 128), 128), jnp.float32),
        in_specs=[pl.BlockSpec(memory_space=pl.ANY)],
        out_specs=pl.BlockSpec(memory_space=pl.ANY),
        scratch_shapes=[
            pltpu.VMEM((n_block, depth, block), jnp.bfloat16),
            pltpu.VMEM((n_block, depth, block), jnp.bfloat16),
            pltpu.VMEM((n_wave, 8 * PIECE * lanes, 128), jnp.float32),
            pltpu.VMEM((16 * ROWS, depth), jnp.bfloat16),
            pltpu.VMEM((n_step, 8 * ROWS, width), jnp.float32),
            pltpu.VMEM((n_step, 4 * ROWS, width), jnp.float32),
            pltpu.VMEM((n_step, 2, ROWS // 2, width), jnp.float32),
            pltpu.VMEM((n_step, 2, ROWS, width), jnp.float32),
            pltpu.VMEM((SLOTS, 128 * lanes, 128), jnp.float32),
            pltpu.VMEM((2 * block // n_col * (height // 128), 128), jnp.float32),
            dma((n_wave, 8)),
            dma((2, 4)),
            dma((1,)),
            dma((n_step,)),
            dma((2,)),
            dma((n_step, 2)),
            dma((2,)),
            dma((n_step, 2)),
            dma((1,)),
            dma((SLOTS,)),
        ],
        compiler_params=pltpu.CompilerParams(
            collective_id=0, has_side_effects=True, vmem_limit_bytes=67043328
        ),
    )(u_window.reshape(height * lanes, 128))
    return summed.reshape(2 * block // n_col, n_block, 1, block)


def solution(mesh):
    placed = (P(None, "prow", None, None, "pcol", None),)
    return jax.shard_map(
        on_device,
        mesh=mesh,
        in_specs=placed,
        out_specs=P("pcol", None, "prow", None),
        check_vma=False,
    )
```

```python
import functools

import jax
import jax.numpy as jnp
from jax import lax
from jax.experimental import pallas as pl
from jax.experimental.pallas import tpu as pltpu
from jax.sharding import PartitionSpec as P

MESH = pl.DeviceIdType.MESH
ROWS = 16
PIECE = 8
TURNS = 3
DELAY = (0, 5, 10, 15, 20, 24)
SPLIT = 2
SHIFT = 0
NEVER = 999
SLOTS = 3
LAGS = (1, 2, 4)


def gray(index):
    return index ^ (index >> 1)


def address(row):
    return gray(row // 4) * 4 + gray(row % 4)


def parents(tree):
    order = [(tree + k + 1) % 4 for k in range(4)]
    order = ([(tree - k - 1) % 4 for k in range(4)])[::-1]
    found = {}
    for node in range(1, 16):
        rest = node ^ (1 << tree)
        found[node] = 0 if rest == 0 else node ^ (1 << [d for d in order if rest >> d & 1][0])
    return found


def plans(n_rows, sources):
    trees = [parents(tree) for tree in range(4)]
    taken = set()
    for tree in trees:
        for node, parent in tree.items():
            assert (parent, node) not in taken
            taken.add((parent, node))
    result = []
    for row in range(n_rows):
        into, onward = [], []
        for index, source in enumerate(sources):
            me = address(row) ^ address(source)
            for number, tree in enumerate(trees):
                depth, node = 0, me
                while node:
                    depth, node = depth + 1, tree[node]
                late = DELAY[depth] + SHIFT * index
                into.append((late, index * 4 + number))
                for d in range(4):
                    if tree.get(me ^ (1 << d)) == me:
                        onward.append((late, index * 4 + number, d))
        onward = sorted(onward)
        result.append((sorted(into), onward + [(NEVER, 0, 0)] * (8 - len(onward))))
    return result


def kernel(
    x_ref,
    out_ref,
    high,
    low,
    panel,
    left,
    part,
    fold,
    mid,
    last,
    stage,
    flat,
    in_sem,
    go_sem,
    fold_send,
    fold_recv,
    mid_send,
    mid_recv,
    last_send,
    last_recv,
    out_sem,
    stage_sem,
    *,
    n_row,
    n_col,
):
    p = lax.axis_index("prow")
    q = lax.axis_index("pcol")
    z, c = q // 2, q % 2
    n_block, depth, block = high.shape
    lanes = depth // 128
    per_block = block // 128
    n_stage = n_block * per_block
    n_wave = panel.shape[0]
    n_set = n_wave // (ROWS // PIECE)
    n_step = n_set * SPLIT
    width = part.shape[2]
    half = part.shape[1] // 2
    first_source = n_row - 2
    anchor = n_row * n_block - 2

    x, y = p % 4, p // 4
    near = [
        y * 4 + x + 1 - 2 * (x % 2),
        y * 4 + 3 - x,
        (y + 1 - 2 * (y % 2)) * 4 + x,
        (3 - y) * 4 + x,
    ]
    peer = q + 1 - 2 * c
    up = ((z + 1) % 4) * 2 + c
    down = ((z + 3) % 4) * 2 + c

    def pick(values):
        found = jnp.int32(values[0])
        for k in range(1, n_row):
            found = jnp.where(p == k, jnp.int32(values[k]), found)
        return found

    plan = plans(n_row, (first_source, first_source + 1))
    def schedule(late):
        turn = [late % TURNS == i for i in range(TURNS)]
        return late // TURNS, turn

    def offset_of(piece):
        return pl.multiple_of((piece % 2 * 4 + piece // 2) * (PIECE * lanes), PIECE * lanes)

    into, onward = [], []
    for k in range(8):
        piece = pick([row[0][k][1] for row in plan])
        late = pick([row[0][k][0] for row in plan])
        into.append((piece, offset_of(piece), *schedule(late)))
        piece = pick([row[1][k][1] for row in plan])
        late = pick([row[1][k][0] for row in plan])
        axis = pick([row[1][k][2] for row in plan])
        target = near[0]
        for d in range(1, 4):
            target = jnp.where(axis == d, near[d], target)
        onward.append((piece, offset_of(piece), *schedule(late), target, late < NEVER))

    ahead = -(-(DELAY[-1] + SHIFT + TURNS * (ROWS // PIECE - 1)) // TURNS)
    size = PIECE * lanes

    def piece_ref(u, start):
        return panel.at[u, pl.ds(start, size), :]

    def stage_copy(n):
        slot = n % SLOTS
        return pltpu.make_async_copy(
            x_ref.at[pl.ds(pl.multiple_of(n * (128 * lanes), 128 * lanes), 128 * lanes), :],
            stage.at[slot],
            stage_sem.at[slot],
        )

    for n in range(SLOTS):
        stage_copy(n).start()

    @pl.when(p >= first_source)
    def _():
        def own(u, _):
            for t in range(4):
                piece = (p - first_source) * 4 + t
                start = pl.multiple_of((t % 2 * 4 + (p - first_source) * 2 + t // 2) * size, size)
                row = (n_block - 1) * block + t * 128 + u * PIECE
                pltpu.make_async_copy(
                    x_ref.at[pl.ds(pl.multiple_of(row * lanes, size), size), :],
                    piece_ref(u, start),
                    in_sem.at[u, piece],
                ).start()
            return 0

        lax.fori_loop(0, n_wave, own, 0)

    barrier = pltpu.get_barrier_semaphore()
    partners = [(row, q) for row in near] + [(p, peer), (p, up), (p, down)]
    for partner in partners:
        pl.semaphore_signal(barrier, inc=1, device_id=partner, device_id_type=MESH)
    pl.semaphore_wait(barrier, len(partners))

    def prepare(n, _):
        slot = n % SLOTS
        stage_copy(n).wait()
        row_id = (
            ((n // per_block) * n_row + p - anchor) * block
            + (n % per_block) * 128
            + lax.broadcasted_iota(jnp.int32, (128, 128), 1)
        )
        for j in range(lanes):
            value = stage[slot, pl.ds(j, 128, stride=lanes), :].T
            first_col = (j // per_block * n_col + q) * block + j % per_block * 128
            if j < per_block:
                col_id = first_col + lax.broadcasted_iota(jnp.int32, (128, 128), 0)
                value = jnp.where(row_id <= col_id, value, 0.0)
            top = value.astype(jnp.bfloat16)
            at = (n // per_block, pl.ds(j * 128, 128), pl.ds(pl.multiple_of(n % per_block * 128, 128), 128))
            high[at] = top
            low[at] = (value - top.astype(jnp.float32)).astype(jnp.bfloat16)

        @pl.when(n + SLOTS < n_stage)
        def _():
            stage_copy(n + SLOTS).start()

        return 0

    def relay(slot, i):
        for piece, start, late, turn in into:
            u = slot - late

            @pl.when(turn[i] & (u >= 0) & (u < n_wave))
            def _():
                ref = piece_ref(u, start)
                pltpu.make_async_copy(ref, ref, in_sem.at[u, piece]).wait()

        for k, (piece, start, late, turn, target, _) in enumerate(onward):
            u = slot - late

            @pl.when(turn[i] & (u >= 0) & (u < n_wave))
            def _():
                ref = piece_ref(u, start)
                pltpu.make_async_remote_copy(
                    src_ref=ref,
                    dst_ref=ref,
                    send_sem=go_sem.at[k],
                    recv_sem=in_sem.at[u, piece],
                    device_id=(target, q),
                    device_id_type=MESH,
                ).start()

    def split_panel(s):
        row = lax.broadcasted_iota(jnp.int32, (8 * ROWS, 128), 0)
        place_of, within = row // ROWS, row % ROWS
        row_id = (place_of % 4 * 2 + place_of // 4) * 128 + s * ROWS + within
        for j in range(lanes):
            waves = [
                panel[s * (ROWS // PIECE) + w, pl.ds(j, 8 * PIECE, stride=lanes), :]
                for w in range(ROWS // PIECE)
            ]
            value = jnp.concatenate(
                [wave[g * PIECE : g * PIECE + PIECE] for g in range(8) for wave in waves], 0
            )
            if j < per_block:
                col_id = q * block + j * 128 + lax.broadcasted_iota(jnp.int32, (8 * ROWS, 128), 1)
                value = jnp.where(row_id <= col_id, value, 0.0)
            top = value.astype(jnp.bfloat16)
            left[: 8 * ROWS, j * 128 : j * 128 + 128] = top
            left[8 * ROWS :, j * 128 : j * 128 + 128] = (value - top.astype(jnp.float32)).astype(
                jnp.bfloat16
            )

    def fold_copy(t):
        return pltpu.make_async_remote_copy(
            src_ref=part.at[t, pl.ds(pl.multiple_of((1 - c) * half, half), half), :],
            dst_ref=fold.at[t],
            send_sem=fold_send.at[0],
            recv_sem=fold_recv.at[t],
            device_id=(p, peer),
            device_id_type=MESH,
        )

    def rows_of(zone, offset):
        return pl.multiple_of(c * half + zone * ROWS + offset, 8)

    def mid_copy(t, way):
        start = rows_of((z + 2) % 4, way * (ROWS // 2))
        return pltpu.make_async_remote_copy(
            src_ref=part.at[t, pl.ds(start, ROWS // 2), :],
            dst_ref=mid.at[t, way],
            send_sem=mid_send.at[way],
            recv_sem=mid_recv.at[t, way],
            device_id=(p, (up, down)[way]),
            device_id_type=MESH,
        )

    def last_copy(t, way):
        start = rows_of((z + (1, 3)[way]) % 4, 0)
        return pltpu.make_async_remote_copy(
            src_ref=part.at[t, pl.ds(start, ROWS), :],
            dst_ref=last.at[t, way],
            send_sem=last_send.at[way],
            recv_sem=last_recv.at[t, way],
            device_id=(p, (up, down)[way]),
            device_id_type=MESH,
        )

    def out_copy(s):
        rows = ROWS * n_block * per_block
        ref = pl.ds(pl.multiple_of(s * rows, rows), rows)
        return pltpu.make_async_copy(flat.at[ref, :], out_ref.at[ref, :], out_sem.at[0])

    def compute(t, h, i):
        at = h * (n_block // SPLIT) + i
        both = jnp.dot(left[...], high[at], preferred_element_type=jnp.float32)
        rest = jnp.dot(left[: 8 * ROWS], low[at], preferred_element_type=jnp.float32)
        part[t, :, i * block : (i + 1) * block] = both[: 8 * ROWS] + both[8 * ROWS :] + rest

    def add_fold(t):
        fold_copy(t).wait_recv()
        for r in range(0, half, 8):
            at = (t, pl.ds(pl.multiple_of(c * half + r, 8), 8), slice(None))
            part[at] = part[at] + fold[t, r : r + 8, :]
        for way in range(2):
            mid_copy(t, way).start()

    def add_mid(t):
        for way in range(2):
            mid_copy(t, way).wait_recv()
            at = (t, pl.ds(rows_of((z + (1, 3)[way]) % 4, way * (ROWS // 2)), ROWS // 2), slice(None))
            part[at] = part[at] + mid[t, way]
        for way in range(2):
            last_copy(t, way).start()

    def add_last(t):
        for way in range(2):
            last_copy(t, way).wait_recv()
        s, h = t // SPLIT, t % SPLIT
        for j in range(width // 128):
            cols = slice(j * 128, j * 128 + 128)
            value = part[t, pl.ds(rows_of(z, 0), ROWS), cols] + last[t, 0, :, cols] + last[t, 1, :, cols]
            first = s * (ROWS * n_block * per_block) + h * (width // 128) + j
            flat[pl.ds(first, ROWS, stride=n_block * per_block), :] = value

        @pl.when(h == SPLIT - 1)
        def _():
            out_copy(s).start()

    share = -(-n_stage // (ahead * TURNS))

    def fill(slot, _):
        for i in range(TURNS):
            relay(slot, i)
            first = (slot * TURNS + i) * share
            lax.fori_loop(first, jnp.minimum(first + share, n_stage), prepare, 0)
        return 0

    lax.fori_loop(0, ahead, fill, 0)

    def sums(t, work, lag):
        @pl.when((t >= lag) & (t < n_step + lag))
        def _():
            work(t - lag)

    def one_set(s, _):
        for h in range(SPLIT):
            t = s * SPLIT + h
            for i in range(TURNS):
                relay(t + ahead, i)
                if h == 0 and i == 0:
                    split_panel(s)
                compute(t, h, i)
                if i == 1:
                    sums(t, add_fold, LAGS[0])
            fold_copy(t).start()
            sums(t, add_mid, LAGS[1])
            sums(t, add_last, LAGS[2])
        return 0

    lax.fori_loop(0, n_set, one_set, 0)

    def drain(t, _):
        for work, lag in zip((add_fold, add_mid, add_last), LAGS):
            sums(t, work, lag)
        return 0

    lax.fori_loop(n_step, n_step + LAGS[2], drain, 0)
    pltpu.make_async_copy(fold, fold, fold_send.at[0]).wait()
    for way in range(2):
        ref = mid.at[:, way]
        pltpu.make_async_copy(ref, ref, mid_send.at[way]).wait()
        ref = last.at[:, way]
        pltpu.make_async_copy(ref, ref, last_send.at[way]).wait()
    ref = panel.at[:, pl.ds(0, size), :]
    for k in range(8):

        @pl.when(onward[k][5])
        def _():
            pltpu.make_async_copy(ref, ref, go_sem.at[k]).wait()

    pltpu.make_async_copy(flat, flat, out_sem.at[0]).wait()


def handed_on(flat):
    def body(flat_ref, out_ref, sems):
        rows = flat_ref.shape[0] // 4
        copies = []
        for k in range(4):
            ref = pl.ds(k * rows, rows)
            copies.append(pltpu.make_async_copy(flat_ref.at[ref, :], out_ref.at[ref, :], sems.at[k]))
            copies[k].start()
        for copy in copies:
            copy.wait()

    return pl.pallas_call(
        body,
        out_shape=jax.ShapeDtypeStruct(flat.shape, flat.dtype),
        in_specs=[pl.BlockSpec(memory_space=pltpu.VMEM)],
        out_specs=pl.BlockSpec(memory_space=pl.ANY),
        scratch_shapes=[pltpu.SemaphoreType.DMA((4,))],
        compiler_params=pltpu.CompilerParams(vmem_limit_bytes=4 * 1024 * 1024),
    )(flat)


def on_device(u_window):
    n_block, _, block, col_blocks, _, _ = u_window.shape
    n_row, n_col = lax.axis_size("prow"), lax.axis_size("pcol")
    depth = col_blocks * block
    lanes = depth // 128
    height = n_block * block
    width = height // SPLIT
    n_set = 128 // ROWS
    n_step = n_set * SPLIT
    n_wave = n_set * (ROWS // PIECE)
    dma = pltpu.SemaphoreType.DMA
    summed = pl.pallas_call(
        functools.partial(kernel, n_row=n_row, n_col=n_col),
        out_shape=jax.ShapeDtypeStruct((2 * block // n_col * (height // 128), 128), jnp.float32),
        in_specs=[pl.BlockSpec(memory_space=pl.ANY)],
        out_specs=pl.BlockSpec(memory_space=pl.ANY),
        scratch_shapes=[
            pltpu.VMEM((n_block, depth, block), jnp.bfloat16),
            pltpu.VMEM((n_block, depth, block), jnp.bfloat16),
            pltpu.VMEM((n_wave, 8 * PIECE * lanes, 128), jnp.float32),
            pltpu.VMEM((16 * ROWS, depth), jnp.bfloat16),
            pltpu.VMEM((n_step, 8 * ROWS, width), jnp.float32),
            pltpu.VMEM((n_step, 4 * ROWS, width), jnp.float32),
            pltpu.VMEM((n_step, 2, ROWS // 2, width), jnp.float32),
            pltpu.VMEM((n_step, 2, ROWS, width), jnp.float32),
            pltpu.VMEM((SLOTS, 128 * lanes, 128), jnp.float32),
            pltpu.VMEM((2 * block // n_col * (height // 128), 128), jnp.float32),
            dma((n_wave, 8)),
            dma((8,)),
            dma((1,)),
            dma((n_step,)),
            dma((2,)),
            dma((n_step, 2)),
            dma((2,)),
            dma((n_step, 2)),
            dma((1,)),
            dma((SLOTS,)),
        ],
        compiler_params=pltpu.CompilerParams(
            collective_id=0, has_side_effects=True, vmem_limit_bytes=67043328
        ),
    )(u_window.reshape(height * lanes, 128))
    summed = handed_on(summed)
    return summed.reshape(2 * block // n_col, n_block, 1, block)


def solution(mesh):
    placed = (P(None, "prow", None, None, "pcol", None),)
    return jax.shard_map(
        on_device,
        mesh=mesh,
        in_specs=placed,
        out_specs=P("pcol", None, "prow", None),
        check_vma=False,
    )
```

```python
import functools

import jax
import jax.numpy as jnp
from jax import lax
from jax.experimental import pallas as pl
from jax.experimental.pallas import tpu as pltpu
from jax.sharding import PartitionSpec as P

MESH = pl.DeviceIdType.MESH
ROWS = 16
PIECE = 8
TURNS = 3
DELAY = (0, 5, 10, 15, 20, 24)
SPLIT = 2
SHIFT = 0
NEVER = 999
SLOTS = 3
LAGS = (1, 2, 5)


def gray(index):
    return index ^ (index >> 1)


def address(row):
    return gray(row // 4) * 4 + gray(row % 4)


def parents(tree):
    order = [(tree + k + 1) % 4 for k in range(4)]
    order = ([(tree - k - 1) % 4 for k in range(4)])[::-1]
    found = {}
    for node in range(1, 16):
        rest = node ^ (1 << tree)
        found[node] = 0 if rest == 0 else node ^ (1 << [d for d in order if rest >> d & 1][0])
    return found


def plans(n_rows, sources):
    trees = [parents(tree) for tree in range(4)]
    taken = set()
    for tree in trees:
        for node, parent in tree.items():
            assert (parent, node) not in taken
            taken.add((parent, node))
    result = []
    for row in range(n_rows):
        into, onward = [], []
        for index, source in enumerate(sources):
            me = address(row) ^ address(source)
            for number, tree in enumerate(trees):
                depth, node = 0, me
                while node:
                    depth, node = depth + 1, tree[node]
                late = DELAY[depth] + SHIFT * index
                into.append((late, index * 4 + number))
                for d in range(4):
                    if tree.get(me ^ (1 << d)) == me:
                        onward.append((late, index * 4 + number, d))
        onward = sorted(onward)
        result.append((sorted(into), onward + [(NEVER, 0, 0)] * (8 - len(onward))))
    return result


def kernel(
    x_ref,
    out_ref,
    high,
    low,
    panel,
    left,
    part,
    fold,
    mid,
    last,
    stage,
    flat,
    in_sem,
    go_sem,
    fold_send,
    fold_recv,
    mid_send,
    mid_recv,
    last_send,
    last_recv,
    out_sem,
    stage_sem,
    *,
    n_row,
    n_col,
):
    p = lax.axis_index("prow")
    q = lax.axis_index("pcol")
    z, c = q // 2, q % 2
    n_block, depth, block = high.shape
    lanes = depth // 128
    per_block = block // 128
    n_stage = n_block * per_block
    n_wave = panel.shape[0]
    n_set = n_wave // (ROWS // PIECE)
    n_step = n_set * SPLIT
    width = part.shape[2]
    half = part.shape[1] // 2
    first_source = n_row - 2
    anchor = n_row * n_block - 2

    x, y = p % 4, p // 4
    near = [
        y * 4 + x + 1 - 2 * (x % 2),
        y * 4 + 3 - x,
        (y + 1 - 2 * (y % 2)) * 4 + x,
        (3 - y) * 4 + x,
    ]
    peer = q + 1 - 2 * c
    up = ((z + 1) % 4) * 2 + c
    down = ((z + 3) % 4) * 2 + c

    barrier = pltpu.get_barrier_semaphore()
    partners = [(row, q) for row in near] + [(p, peer), (p, up), (p, down)]
    for partner in partners:
        pl.semaphore_signal(barrier, inc=1, device_id=partner, device_id_type=MESH)

    def pick(values):
        found = jnp.int32(values[0])
        for k in range(1, n_row):
            found = jnp.where(p == k, jnp.int32(values[k]), found)
        return found

    plan = plans(n_row, (first_source, first_source + 1))
    def schedule(late):
        turn = [late % TURNS == i for i in range(TURNS)]
        return late // TURNS, turn

    def offset_of(piece):
        return pl.multiple_of((piece % 2 * 4 + piece // 2) * (PIECE * lanes), PIECE * lanes)

    into, onward = [], []
    for k in range(8):
        piece = pick([row[0][k][1] for row in plan])
        late = pick([row[0][k][0] for row in plan])
        into.append((piece, offset_of(piece), *schedule(late)))
        piece = pick([row[1][k][1] for row in plan])
        late = pick([row[1][k][0] for row in plan])
        axis = pick([row[1][k][2] for row in plan])
        target = near[0]
        for d in range(1, 4):
            target = jnp.where(axis == d, near[d], target)
        onward.append((piece, offset_of(piece), *schedule(late), target, late < NEVER))

    ahead = -(-(DELAY[-1] + SHIFT + TURNS * (ROWS // PIECE - 1)) // TURNS)
    size = PIECE * lanes

    def piece_ref(u, start):
        return panel.at[u, pl.ds(start, size), :]

    def stage_copy(n):
        slot = n % SLOTS
        return pltpu.make_async_copy(
            x_ref.at[pl.ds(pl.multiple_of(n * (128 * lanes), 128 * lanes), 128 * lanes), :],
            stage.at[slot],
            stage_sem.at[slot],
        )

    for n in range(SLOTS):
        stage_copy(n).start()

    @pl.when(p >= first_source)
    def _():
        def own(u, _):
            for t in range(4):
                piece = (p - first_source) * 4 + t
                start = pl.multiple_of((t % 2 * 4 + (p - first_source) * 2 + t // 2) * size, size)
                row = (n_block - 1) * block + t * 128 + u * PIECE
                pltpu.make_async_copy(
                    x_ref.at[pl.ds(pl.multiple_of(row * lanes, size), size), :],
                    piece_ref(u, start),
                    in_sem.at[u, piece],
                ).start()
            return 0

        lax.fori_loop(0, n_wave, own, 0)

    pl.semaphore_wait(barrier, len(partners))

    def prepare(n, _):
        slot = n % SLOTS
        stage_copy(n).wait()
        row_id = (
            ((n // per_block) * n_row + p - anchor) * block
            + (n % per_block) * 128
            + lax.broadcasted_iota(jnp.int32, (128, 128), 1)
        )
        for j in range(lanes):
            value = stage[slot, pl.ds(j, 128, stride=lanes), :].T
            first_col = (j // per_block * n_col + q) * block + j % per_block * 128
            if j < per_block:
                col_id = first_col + lax.broadcasted_iota(jnp.int32, (128, 128), 0)
                value = jnp.where(row_id <= col_id, value, 0.0)
            top = value.astype(jnp.bfloat16)
            at = (n // per_block, pl.ds(j * 128, 128), pl.ds(pl.multiple_of(n % per_block * 128, 128), 128))
            high[at] = top
            low[at] = (value - top.astype(jnp.float32)).astype(jnp.bfloat16)

        @pl.when(n + SLOTS < n_stage)
        def _():
            stage_copy(n + SLOTS).start()

        return 0

    def relay(slot, i):
        for piece, start, late, turn in into:
            u = slot - late

            @pl.when(turn[i] & (u >= 0) & (u < n_wave))
            def _():
                ref = piece_ref(u, start)
                pltpu.make_async_copy(ref, ref, in_sem.at[u, piece]).wait()

        for k, (piece, start, late, turn, target, _) in enumerate(onward):
            u = slot - late

            @pl.when(turn[i] & (u >= 0) & (u < n_wave))
            def _():
                ref = piece_ref(u, start)
                pltpu.make_async_remote_copy(
                    src_ref=ref,
                    dst_ref=ref,
                    send_sem=go_sem.at[k],
                    recv_sem=in_sem.at[u, piece],
                    device_id=(target, q),
                    device_id_type=MESH,
                ).start()

    def split_panel(s):
        row = lax.broadcasted_iota(jnp.int32, (8 * ROWS, 128), 0)
        place_of, within = row // ROWS, row % ROWS
        row_id = (place_of % 4 * 2 + place_of // 4) * 128 + s * ROWS + within
        for j in range(lanes):
            waves = [
                panel[s * (ROWS // PIECE) + w, pl.ds(j, 8 * PIECE, stride=lanes), :]
                for w in range(ROWS // PIECE)
            ]
            value = jnp.concatenate(
                [wave[g * PIECE : g * PIECE + PIECE] for g in range(8) for wave in waves], 0
            )
            if j < per_block:
                col_id = q * block + j * 128 + lax.broadcasted_iota(jnp.int32, (8 * ROWS, 128), 1)
                value = jnp.where(row_id <= col_id, value, 0.0)
            top = value.astype(jnp.bfloat16)
            left[: 8 * ROWS, j * 128 : j * 128 + 128] = top
            left[8 * ROWS :, j * 128 : j * 128 + 128] = (value - top.astype(jnp.float32)).astype(
                jnp.bfloat16
            )

    def fold_copy(t):
        return pltpu.make_async_remote_copy(
            src_ref=part.at[t, pl.ds(pl.multiple_of((1 - c) * half, half), half), :],
            dst_ref=fold.at[t],
            send_sem=fold_send.at[0],
            recv_sem=fold_recv.at[t],
            device_id=(p, peer),
            device_id_type=MESH,
        )

    def rows_of(zone, offset):
        return pl.multiple_of(c * half + zone * ROWS + offset, 8)

    def mid_copy(t, way):
        start = rows_of((z + 2) % 4, way * (ROWS // 2))
        return pltpu.make_async_remote_copy(
            src_ref=part.at[t, pl.ds(start, ROWS // 2), :],
            dst_ref=mid.at[t, way],
            send_sem=mid_send.at[way],
            recv_sem=mid_recv.at[t, way],
            device_id=(p, (up, down)[way]),
            device_id_type=MESH,
        )

    def last_copy(t, way):
        start = rows_of((z + (1, 3)[way]) % 4, 0)
        return pltpu.make_async_remote_copy(
            src_ref=part.at[t, pl.ds(start, ROWS), :],
            dst_ref=last.at[t, way],
            send_sem=last_send.at[way],
            recv_sem=last_recv.at[t, way],
            device_id=(p, (up, down)[way]),
            device_id_type=MESH,
        )

    def out_copy(s):
        rows = ROWS * n_block * per_block
        ref = pl.ds(pl.multiple_of(s * rows, rows), rows)
        return pltpu.make_async_copy(flat.at[ref, :], out_ref.at[ref, :], out_sem.at[0])

    def compute(t, h, i):
        at = h * (n_block // SPLIT) + i
        both = jnp.dot(left[...], high[at], preferred_element_type=jnp.float32)
        rest = jnp.dot(left[: 8 * ROWS], low[at], preferred_element_type=jnp.float32)
        part[t, :, i * block : (i + 1) * block] = both[: 8 * ROWS] + both[8 * ROWS :] + rest

    def add_fold(t):
        fold_copy(t).wait_recv()
        for r in range(0, half, 8):
            at = (t, pl.ds(pl.multiple_of(c * half + r, 8), 8), slice(None))
            part[at] = part[at] + fold[t, r : r + 8, :]
        for way in range(2):
            mid_copy(t, way).start()

    def add_mid(t):
        for way in range(2):
            mid_copy(t, way).wait_recv()
            at = (t, pl.ds(rows_of((z + (1, 3)[way]) % 4, way * (ROWS // 2)), ROWS // 2), slice(None))
            part[at] = part[at] + mid[t, way]
        for way in range(2):
            last_copy(t, way).start()

    def add_last(t):
        for way in range(2):
            last_copy(t, way).wait_recv()
        s, h = t // SPLIT, t % SPLIT
        for j in range(width // 128):
            cols = slice(j * 128, j * 128 + 128)
            value = part[t, pl.ds(rows_of(z, 0), ROWS), cols] + last[t, 0, :, cols] + last[t, 1, :, cols]
            first = s * (ROWS * n_block * per_block) + h * (width // 128) + j
            flat[pl.ds(first, ROWS, stride=n_block * per_block), :] = value

        @pl.when(h == SPLIT - 1)
        def _():
            out_copy(s).start()

    share = -(-n_stage // (ahead * TURNS))

    def fill(slot, _):
        for i in range(TURNS):
            relay(slot, i)
            first = (slot * TURNS + i) * share
            lax.fori_loop(first, jnp.minimum(first + share, n_stage), prepare, 0)
        return 0

    lax.fori_loop(0, ahead, fill, 0)

    def sums(t, work, lag):
        @pl.when((t >= lag) & (t < n_step + lag))
        def _():
            work(t - lag)

    def one_set(s, _):
        for h in range(SPLIT):
            t = s * SPLIT + h
            for i in range(TURNS):
                relay(t + ahead, i)
                if h == 0 and i == 0:
                    split_panel(s)
                compute(t, h, i)
                if i == 1:
                    sums(t, add_fold, LAGS[0])
            fold_copy(t).start()
            sums(t, add_mid, LAGS[1])
            sums(t, add_last, LAGS[2])
        return 0

    lax.fori_loop(0, n_set, one_set, 0)

    def drain(t, _):
        for work, lag in zip((add_fold, add_mid, add_last), LAGS):
            sums(t, work, lag)
        return 0

    lax.fori_loop(n_step, n_step + LAGS[2], drain, 0)
    pltpu.make_async_copy(fold, fold, fold_send.at[0]).wait()
    for way in range(2):
        ref = mid.at[:, way]
        pltpu.make_async_copy(ref, ref, mid_send.at[way]).wait()
        ref = last.at[:, way]
        pltpu.make_async_copy(ref, ref, last_send.at[way]).wait()
    ref = panel.at[:, pl.ds(0, size), :]
    for k in range(8):

        @pl.when(onward[k][5])
        def _():
            pltpu.make_async_copy(ref, ref, go_sem.at[k]).wait()

    pltpu.make_async_copy(flat, flat, out_sem.at[0]).wait()


def handed_on(flat):
    parts = 4
    rows = flat.shape[0] // parts

    def body(flat_ref, out_ref, held, in_sem, out_sem):
        def take(k):
            ref = pl.ds(k * rows, rows)
            return pltpu.make_async_copy(flat_ref.at[ref, :], held.at[ref, :], in_sem.at[k])

        def give(k):
            ref = pl.ds(k * rows, rows)
            return pltpu.make_async_copy(held.at[ref, :], out_ref.at[ref, :], out_sem.at[k])

        for k in range(parts):
            take(k).start()
        for k in range(parts):
            take(k).wait()
            give(k).start()
        for k in range(parts):
            give(k).wait()

    return pl.pallas_call(
        body,
        out_shape=jax.ShapeDtypeStruct(flat.shape, flat.dtype),
        in_specs=[pl.BlockSpec(memory_space=pl.ANY)],
        out_specs=pl.BlockSpec(memory_space=pl.ANY),
        scratch_shapes=[
            pltpu.VMEM(flat.shape, flat.dtype),
            pltpu.SemaphoreType.DMA((parts,)),
            pltpu.SemaphoreType.DMA((parts,)),
        ],
    )(flat)


def on_device(u_window):
    n_block, _, block, col_blocks, _, _ = u_window.shape
    n_row, n_col = lax.axis_size("prow"), lax.axis_size("pcol")
    depth = col_blocks * block
    lanes = depth // 128
    height = n_block * block
    width = height // SPLIT
    n_set = 128 // ROWS
    n_step = n_set * SPLIT
    n_wave = n_set * (ROWS // PIECE)
    dma = pltpu.SemaphoreType.DMA
    summed = pl.pallas_call(
        functools.partial(kernel, n_row=n_row, n_col=n_col),
        out_shape=jax.ShapeDtypeStruct((2 * block // n_col * (height // 128), 128), jnp.float32),
        in_specs=[pl.BlockSpec(memory_space=pl.ANY)],
        out_specs=pl.BlockSpec(memory_space=pl.ANY),
        scratch_shapes=[
            pltpu.VMEM((n_block, depth, block), jnp.bfloat16),
            pltpu.VMEM((n_block, depth, block), jnp.bfloat16),
            pltpu.VMEM((n_wave, 8 * PIECE * lanes, 128), jnp.float32),
            pltpu.VMEM((16 * ROWS, depth), jnp.bfloat16),
            pltpu.VMEM((n_step, 8 * ROWS, width), jnp.float32),
            pltpu.VMEM((n_step, 4 * ROWS, width), jnp.float32),
            pltpu.VMEM((n_step, 2, ROWS // 2, width), jnp.float32),
            pltpu.VMEM((n_step, 2, ROWS, width), jnp.float32),
            pltpu.VMEM((SLOTS, 128 * lanes, 128), jnp.float32),
            pltpu.VMEM((2 * block // n_col * (height // 128), 128), jnp.float32),
            dma((n_wave, 8)),
            dma((8,)),
            dma((1,)),
            dma((n_step,)),
            dma((2,)),
            dma((n_step, 2)),
            dma((2,)),
            dma((n_step, 2)),
            dma((1,)),
            dma((SLOTS,)),
        ],
        compiler_params=pltpu.CompilerParams(
            collective_id=0, has_side_effects=True, vmem_limit_bytes=67043328
        ),
    )(u_window.reshape(height * lanes, 128))
    summed = handed_on(summed)
    return summed.reshape(2 * block // n_col, n_block, 1, block)


def solution(mesh):
    placed = (P(None, "prow", None, None, "pcol", None),)
    return jax.shard_map(
        on_device,
        mesh=mesh,
        in_specs=placed,
        out_specs=P("pcol", None, "prow", None),
        check_vma=False,
    )
```

```python
import functools

import jax
import jax.numpy as jnp
from jax import lax
from jax.experimental import pallas as pl
from jax.experimental.pallas import tpu as pltpu
from jax.sharding import PartitionSpec as P

MESH = pl.DeviceIdType.MESH
ROWS = 16
PIECE = 8
TURNS = 3
DELAY = (0, 5, 10, 15, 20, 24)
SPLIT = 2
SHIFT = 0
NEVER = 999
SLOTS = 3
LAGS = (1, 2, 5)


def gray(index):
    return index ^ (index >> 1)


def address(row):
    return gray(row // 4) * 4 + gray(row % 4)


def parents(tree):
    order = [(tree + k + 1) % 4 for k in range(4)]
    order = ([(tree - k - 1) % 4 for k in range(4)])[::-1]
    found = {}
    for node in range(1, 16):
        rest = node ^ (1 << tree)
        found[node] = 0 if rest == 0 else node ^ (1 << [d for d in order if rest >> d & 1][0])
    return found


def plans(n_rows, sources):
    trees = [parents(tree) for tree in range(4)]
    taken = set()
    for tree in trees:
        for node, parent in tree.items():
            assert (parent, node) not in taken
            taken.add((parent, node))
    result = []
    for row in range(n_rows):
        into, onward = [], []
        for index, source in enumerate(sources):
            me = address(row) ^ address(source)
            for number, tree in enumerate(trees):
                depth, node = 0, me
                while node:
                    depth, node = depth + 1, tree[node]
                late = DELAY[depth] + SHIFT * index
                into.append((late, index * 4 + number))
                for d in range(4):
                    if tree.get(me ^ (1 << d)) == me:
                        onward.append((late, index * 4 + number, d))
        onward = sorted(onward)
        result.append((sorted(into), onward + [(NEVER, 0, 0)] * (8 - len(onward))))
    return result


def kernel(
    x_ref,
    out_ref,
    high,
    low,
    panel,
    left,
    part,
    fold,
    mid,
    last,
    stage,
    flat,
    in_sem,
    go_sem,
    fold_send,
    fold_recv,
    mid_send,
    mid_recv,
    last_send,
    last_recv,
    out_sem,
    stage_sem,
    *,
    n_row,
    n_col,
):
    p = lax.axis_index("prow")
    q = lax.axis_index("pcol")
    z, c = q // 2, q % 2
    n_block, depth, block = high.shape
    lanes = depth // 128
    per_block = block // 128
    n_stage = n_block * per_block
    n_wave = panel.shape[0]
    n_set = n_wave // (ROWS // PIECE)
    n_step = n_set * SPLIT
    width = part.shape[2]
    half = part.shape[1] // 2
    first_source = n_row - 2
    anchor = n_row * n_block - 2

    x, y = p % 4, p // 4
    near = [
        y * 4 + x + 1 - 2 * (x % 2),
        y * 4 + 3 - x,
        (y + 1 - 2 * (y % 2)) * 4 + x,
        (3 - y) * 4 + x,
    ]
    peer = q + 1 - 2 * c
    up = ((z + 1) % 4) * 2 + c
    down = ((z + 3) % 4) * 2 + c

    barrier = pltpu.get_barrier_semaphore()
    partners = [(row, q) for row in near] + [(p, peer), (p, up), (p, down)]
    for partner in partners:
        pl.semaphore_signal(barrier, inc=1, device_id=partner, device_id_type=MESH)

    def pick(values):
        found = jnp.int32(values[0])
        for k in range(1, n_row):
            found = jnp.where(p == k, jnp.int32(values[k]), found)
        return found

    plan = plans(n_row, (first_source, first_source + 1))
    def schedule(late):
        turn = [late % TURNS == i for i in range(TURNS)]
        return late // TURNS, turn

    def offset_of(piece):
        return pl.multiple_of((piece % 2 * 4 + piece // 2) * (PIECE * lanes), PIECE * lanes)

    into, onward = [], []
    for k in range(8):
        piece = pick([row[0][k][1] for row in plan])
        late = pick([row[0][k][0] for row in plan])
        into.append((piece, offset_of(piece), *schedule(late)))
        piece = pick([row[1][k][1] for row in plan])
        late = pick([row[1][k][0] for row in plan])
        axis = pick([row[1][k][2] for row in plan])
        target = near[0]
        for d in range(1, 4):
            target = jnp.where(axis == d, near[d], target)
        onward.append((piece, offset_of(piece), *schedule(late), target, late < NEVER))

    ahead = -(-(DELAY[-1] + SHIFT + TURNS * (ROWS // PIECE - 1)) // TURNS)
    size = PIECE * lanes

    def piece_ref(u, start):
        return panel.at[u, pl.ds(start, size), :]

    def stage_copy(n):
        slot = n % SLOTS
        return pltpu.make_async_copy(
            x_ref.at[pl.ds(pl.multiple_of(n * (128 * lanes), 128 * lanes), 128 * lanes), :],
            stage.at[slot],
            stage_sem.at[slot],
        )

    @pl.when(p >= first_source)
    def _():
        def own(u, _):
            for t in range(4):
                piece = (p - first_source) * 4 + t
                start = pl.multiple_of((t % 2 * 4 + (p - first_source) * 2 + t // 2) * size, size)
                row = (n_block - 1) * block + t * 128 + u * PIECE
                pltpu.make_async_copy(
                    x_ref.at[pl.ds(pl.multiple_of(row * lanes, size), size), :],
                    piece_ref(u, start),
                    in_sem.at[u, piece],
                ).start()
            return 0

        lax.fori_loop(0, n_wave, own, 0)

    for n in range(SLOTS):
        stage_copy(n).start()

    pl.semaphore_wait(barrier, len(partners))

    def prepare(n, _):
        slot = n % SLOTS
        stage_copy(n).wait()
        row_id = (
            ((n // per_block) * n_row + p - anchor) * block
            + (n % per_block) * 128
            + lax.broadcasted_iota(jnp.int32, (128, 128), 1)
        )
        for j in range(lanes):
            value = stage[slot, pl.ds(j, 128, stride=lanes), :].T
            first_col = (j // per_block * n_col + q) * block + j % per_block * 128
            if j < per_block:
                col_id = first_col + lax.broadcasted_iota(jnp.int32, (128, 128), 0)
                value = jnp.where(row_id <= col_id, value, 0.0)
            top = value.astype(jnp.bfloat16)
            at = (n // per_block, pl.ds(j * 128, 128), pl.ds(pl.multiple_of(n % per_block * 128, 128), 128))
            high[at] = top
            low[at] = (value - top.astype(jnp.float32)).astype(jnp.bfloat16)

        @pl.when(n + SLOTS < n_stage)
        def _():
            stage_copy(n + SLOTS).start()

        return 0

    def relay(slot, i):
        for piece, start, late, turn in into:
            u = slot - late

            @pl.when(turn[i] & (u >= 0) & (u < n_wave))
            def _():
                ref = piece_ref(u, start)
                pltpu.make_async_copy(ref, ref, in_sem.at[u, piece]).wait()

        for k, (piece, start, late, turn, target, _) in enumerate(onward):
            u = slot - late

            @pl.when(turn[i] & (u >= 0) & (u < n_wave))
            def _():
                ref = piece_ref(u, start)
                pltpu.make_async_remote_copy(
                    src_ref=ref,
                    dst_ref=ref,
                    send_sem=go_sem.at[k],
                    recv_sem=in_sem.at[u, piece],
                    device_id=(target, q),
                    device_id_type=MESH,
                ).start()

    def split_panel(s):
        row = lax.broadcasted_iota(jnp.int32, (8 * ROWS, 128), 0)
        place_of, within = row // ROWS, row % ROWS
        row_id = (place_of % 4 * 2 + place_of // 4) * 128 + s * ROWS + within
        for j in range(lanes):
            waves = [
                panel[s * (ROWS // PIECE) + w, pl.ds(j, 8 * PIECE, stride=lanes), :]
                for w in range(ROWS // PIECE)
            ]
            value = jnp.concatenate(
                [wave[g * PIECE : g * PIECE + PIECE] for g in range(8) for wave in waves], 0
            )
            if j < per_block:
                col_id = q * block + j * 128 + lax.broadcasted_iota(jnp.int32, (8 * ROWS, 128), 1)
                value = jnp.where(row_id <= col_id, value, 0.0)
            top = value.astype(jnp.bfloat16)
            left[: 8 * ROWS, j * 128 : j * 128 + 128] = top
            left[8 * ROWS :, j * 128 : j * 128 + 128] = (value - top.astype(jnp.float32)).astype(
                jnp.bfloat16
            )

    def fold_copy(t):
        return pltpu.make_async_remote_copy(
            src_ref=part.at[t, pl.ds(pl.multiple_of((1 - c) * half, half), half), :],
            dst_ref=fold.at[t],
            send_sem=fold_send.at[0],
            recv_sem=fold_recv.at[t],
            device_id=(p, peer),
            device_id_type=MESH,
        )

    def rows_of(zone, offset):
        return pl.multiple_of(c * half + zone * ROWS + offset, 8)

    def mid_copy(t, way):
        start = rows_of((z + 2) % 4, way * (ROWS // 2))
        return pltpu.make_async_remote_copy(
            src_ref=part.at[t, pl.ds(start, ROWS // 2), :],
            dst_ref=mid.at[t, way],
            send_sem=mid_send.at[way],
            recv_sem=mid_recv.at[t, way],
            device_id=(p, (up, down)[way]),
            device_id_type=MESH,
        )

    def last_copy(t, way):
        start = rows_of((z + (1, 3)[way]) % 4, 0)
        return pltpu.make_async_remote_copy(
            src_ref=part.at[t, pl.ds(start, ROWS), :],
            dst_ref=last.at[t, way],
            send_sem=last_send.at[way],
            recv_sem=last_recv.at[t, way],
            device_id=(p, (up, down)[way]),
            device_id_type=MESH,
        )

    def out_copy(s):
        rows = ROWS * n_block * per_block
        ref = pl.ds(pl.multiple_of(s * rows, rows), rows)
        return pltpu.make_async_copy(flat.at[ref, :], out_ref.at[ref, :], out_sem.at[0])

    def compute(t, h, i):
        at = h * (n_block // SPLIT) + i
        both = jnp.dot(left[...], high[at], preferred_element_type=jnp.float32)
        rest = jnp.dot(left[: 8 * ROWS], low[at], preferred_element_type=jnp.float32)
        part[t, :, i * block : (i + 1) * block] = both[: 8 * ROWS] + both[8 * ROWS :] + rest

    def add_fold(t):
        fold_copy(t).wait_recv()
        for r in range(0, half, 8):
            at = (t, pl.ds(pl.multiple_of(c * half + r, 8), 8), slice(None))
            part[at] = part[at] + fold[t, r : r + 8, :]
        for way in range(2):
            mid_copy(t, way).start()

    def add_mid(t):
        for way in range(2):
            mid_copy(t, way).wait_recv()
            at = (t, pl.ds(rows_of((z + (1, 3)[way]) % 4, way * (ROWS // 2)), ROWS // 2), slice(None))
            part[at] = part[at] + mid[t, way]
        for way in range(2):
            last_copy(t, way).start()

    def add_last(t):
        for way in range(2):
            last_copy(t, way).wait_recv()
        s, h = t // SPLIT, t % SPLIT
        for j in range(width // 128):
            cols = slice(j * 128, j * 128 + 128)
            value = part[t, pl.ds(rows_of(z, 0), ROWS), cols] + last[t, 0, :, cols] + last[t, 1, :, cols]
            first = s * (ROWS * n_block * per_block) + h * (width // 128) + j
            flat[pl.ds(first, ROWS, stride=n_block * per_block), :] = value

        @pl.when(h == SPLIT - 1)
        def _():
            out_copy(s).start()

    share = -(-n_stage // (ahead * TURNS))

    def fill(slot, _):
        for i in range(TURNS):
            relay(slot, i)
            first = (slot * TURNS + i) * share
            lax.fori_loop(first, jnp.minimum(first + share, n_stage), prepare, 0)
        return 0

    lax.fori_loop(0, ahead, fill, 0)

    def sums(t, work, lag):
        @pl.when((t >= lag) & (t < n_step + lag))
        def _():
            work(t - lag)

    def one_set(s, _):
        for h in range(SPLIT):
            t = s * SPLIT + h
            for i in range(TURNS):
                relay(t + ahead, i)
                if h == 0 and i == 0:
                    split_panel(s)
                compute(t, h, i)
                if i == 1:
                    sums(t, add_fold, LAGS[0])
            fold_copy(t).start()
            sums(t, add_mid, LAGS[1])
            sums(t, add_last, LAGS[2])
        return 0

    lax.fori_loop(0, n_set, one_set, 0)

    def drain(t, _):
        for work, lag in zip((add_fold, add_mid, add_last), LAGS):
            sums(t, work, lag)
        return 0

    lax.fori_loop(n_step, n_step + LAGS[2], drain, 0)
    pltpu.make_async_copy(fold, fold, fold_send.at[0]).wait()
    for way in range(2):
        ref = mid.at[:, way]
        pltpu.make_async_copy(ref, ref, mid_send.at[way]).wait()
        ref = last.at[:, way]
        pltpu.make_async_copy(ref, ref, last_send.at[way]).wait()
    ref = panel.at[:, pl.ds(0, size), :]
    for k in range(8):

        @pl.when(onward[k][5])
        def _():
            pltpu.make_async_copy(ref, ref, go_sem.at[k]).wait()

    pltpu.make_async_copy(flat, flat, out_sem.at[0]).wait()


def handed_on(flat):
    parts = 4
    rows = flat.shape[0] // parts

    def body(flat_ref, out_ref, held, in_sem, out_sem):
        def take(k):
            ref = pl.ds(k * rows, rows)
            return pltpu.make_async_copy(flat_ref.at[ref, :], held.at[ref, :], in_sem.at[k])

        def give(k):
            ref = pl.ds(k * rows, rows)
            return pltpu.make_async_copy(held.at[ref, :], out_ref.at[ref, :], out_sem.at[k])

        for k in range(parts):
            take(k).start()
        for k in range(parts):
            take(k).wait()
            give(k).start()
        for k in range(parts):
            give(k).wait()

    return pl.pallas_call(
        body,
        out_shape=jax.ShapeDtypeStruct(flat.shape, flat.dtype),
        in_specs=[pl.BlockSpec(memory_space=pl.ANY)],
        out_specs=pl.BlockSpec(memory_space=pl.ANY),
        scratch_shapes=[
            pltpu.VMEM(flat.shape, flat.dtype),
            pltpu.SemaphoreType.DMA((parts,)),
            pltpu.SemaphoreType.DMA((parts,)),
        ],
    )(flat)


def on_device(u_window):
    n_block, _, block, col_blocks, _, _ = u_window.shape
    n_row, n_col = lax.axis_size("prow"), lax.axis_size("pcol")
    depth = col_blocks * block
    lanes = depth // 128
    height = n_block * block
    width = height // SPLIT
    n_set = 128 // ROWS
    n_step = n_set * SPLIT
    n_wave = n_set * (ROWS // PIECE)
    dma = pltpu.SemaphoreType.DMA
    summed = pl.pallas_call(
        functools.partial(kernel, n_row=n_row, n_col=n_col),
        out_shape=jax.ShapeDtypeStruct((2 * block // n_col * (height // 128), 128), jnp.float32),
        in_specs=[pl.BlockSpec(memory_space=pl.ANY)],
        out_specs=pl.BlockSpec(memory_space=pl.ANY),
        scratch_shapes=[
            pltpu.VMEM((n_block, depth, block), jnp.bfloat16),
            pltpu.VMEM((n_block, depth, block), jnp.bfloat16),
            pltpu.VMEM((n_wave, 8 * PIECE * lanes, 128), jnp.float32),
            pltpu.VMEM((16 * ROWS, depth), jnp.bfloat16),
            pltpu.VMEM((n_step, 8 * ROWS, width), jnp.float32),
            pltpu.VMEM((n_step, 4 * ROWS, width), jnp.float32),
            pltpu.VMEM((n_step, 2, ROWS // 2, width), jnp.float32),
            pltpu.VMEM((n_step, 2, ROWS, width), jnp.float32),
            pltpu.VMEM((SLOTS, 128 * lanes, 128), jnp.float32),
            pltpu.VMEM((2 * block // n_col * (height // 128), 128), jnp.float32),
            dma((n_wave, 8)),
            dma((8,)),
            dma((1,)),
            dma((n_step,)),
            dma((2,)),
            dma((n_step, 2)),
            dma((2,)),
            dma((n_step, 2)),
            dma((1,)),
            dma((SLOTS,)),
        ],
        compiler_params=pltpu.CompilerParams(
            collective_id=0, has_side_effects=True, vmem_limit_bytes=67043328
        ),
    )(u_window.reshape(height * lanes, 128))
    summed = handed_on(summed)
    return summed.reshape(2 * block // n_col, n_block, 1, block)


def solution(mesh):
    placed = (P(None, "prow", None, None, "pcol", None),)
    return jax.shard_map(
        on_device,
        mesh=mesh,
        in_specs=placed,
        out_specs=P("pcol", None, "prow", None),
        check_vma=False,
    )
```
